32 devices in a mesh: corpus: 8 (over z, y), neur: 4 (over x, core).
Axes of the slice: x: 2, y: 2, z: 4, core: 2. Of those that a mesh axis runs over, the one named last changes fastest.
Arguments:
- resid: bfloat16 [32768, 4096], P(('corpus', 'neur')), may hold values from -140 to 140
- norm_gain: float32 [4096], replicated, may hold values from 0.1 to 1.9
- w_gate: bfloat16 [4096, 6144], P(None, 'neur'), may hold values from -0.09375 to 0.09375
- w_up: bfloat16 [4096, 6144], P(None, 'neur'), may hold values from -0.09375 to 0.09375
- hit_neuron: int32 [2048], P(('corpus', 'neur')), may hold values from 0 to 6143, as said below
- hit_start: int32 [2048], P(('corpus', 'neur')), may hold values from 0 to 32736, as said below
- hit_mask: int32 [2048, 32], P(('corpus', 'neur')), may hold values from 0 to 1, as said below
Outputs:
- profile: float32 [2048, 32], P(('corpus', 'neur'))
- coact: float32 [2048, 1536], P(('corpus', 'neur'))
The draws below stay inside these ranges and needn't reach their ends.
Inputs may be any that keep to these rules, and one draw needn't show every extreme that they name: `hit_start`: every window of 32 tokens lies inside one aligned block of 1024 corpus tokens. Among the hits of one device (blocks of 64 hits) at most 4 window lies in one such block; this bound is reached by every device in every draw. `hit_neuron`: the hits of block b of 64 hits (blocks in the order corpus+neur) name neurons of block b % 4 of 6144 // 4 neurons. `hit_mask`: the ones of each row form one run that contains positions 15 and 16.
All inputs are finite; a program needn't handle non-finite values.
Results may differ from the reference program's by a relative error of at most 0.0042.
Values may be sent and summed in bfloat16 or wider, within the bound.
No kernel may reach another device: no remote copies, remote signals or barrier semaphores. Data moves between devices by JAX's collectives and lax.ppermute only.
A program may use at most 320 MiB of HBM per device.

```python
import math
import jax
import jax.numpy as jnp
from jax import lax

D = 4096
FF_WIN = 6144
TOK_DEV = 1024
HITS_DEV = 64
WIN = 32
CAP = 4
TOKENS = 32768
HITS = 2048
N_NEUR = 4
DEVICES = 32


def owner_table(key):
    hot_pair = jax.random.permutation(jax.random.fold_in(key, 7), DEVICES)[:2]

    def one_device(device_key):
        device_keys = jax.random.split(device_key, 3)
        hot_owner = hot_pair[jax.random.randint(device_keys[0], (), 0, 2)]
        base_ids = jnp.arange(DEVICES - 1, dtype=jnp.int32)
        other_owners = base_ids + (base_ids >= hot_owner).astype(jnp.int32)
        owner_pool = jnp.repeat(other_owners, CAP)
        chosen = owner_pool[jax.random.permutation(device_keys[1], owner_pool.shape[0])[:HITS_DEV - CAP]]
        listed = jnp.concatenate([jnp.full((CAP,), hot_owner, jnp.int32), chosen.astype(jnp.int32)])
        return listed[jax.random.permutation(device_keys[2], HITS_DEV)]
    return jax.vmap(one_device)(jax.random.split(key, DEVICES)).reshape(-1)


def draw_hit_start(key, part):
    owners = owner_table(jax.random.fold_in(key, 11))
    offsets = jax.random.randint(jax.random.fold_in(key, 12), (HITS,), 0, TOK_DEV - WIN + 1)
    return (owners * TOK_DEV + offsets).astype(jnp.int32)


def draw_hit_neuron(key, part):
    local_width = FF_WIN // N_NEUR
    block_ids = jnp.arange(HITS, dtype=jnp.int32) // HITS_DEV
    chosen = jax.random.randint(jax.random.fold_in(key, 21), (HITS,), 0, local_width)
    return (block_ids % N_NEUR * local_width + chosen).astype(jnp.int32)


def draw_hit_mask(key, part):
    first_live = jax.random.randint(jax.random.fold_in(key, 31), (HITS, 1), 0, WIN // 2)
    last_live = jax.random.randint(jax.random.fold_in(key, 32), (HITS, 1), WIN // 2, WIN)
    position = jnp.arange(WIN, dtype=jnp.int32)[None, :]
    return ((position >= first_live) & (position <= last_live)).astype(jnp.int32)


def draw_resid(key, part):
    draw_keys = jax.random.split(jax.random.fold_in(key, 41), 3)
    row_scale = jnp.exp(jax.random.uniform(draw_keys[0], (TOKENS, 1), minval=0.0, maxval=math.log(10.0)))
    column_scale = jnp.exp(jax.random.uniform(draw_keys[1], (1, D), minval=-1.0, maxval=1.0))
    values = jnp.clip(jax.random.normal(draw_keys[2], (TOKENS, D)), -5.0, 5.0)
    return (values * row_scale * column_scale).astype(jnp.bfloat16)


def block_levels(own_key, shape, cuts, least, top_value):
    def one(dim, shards_of):
        steps = jax.random.uniform(jax.random.fold_in(jax.random.fold_in(own_key, 6), dim), (shards_of,), jnp.float32, least / len(cuts), top_value / len(cuts))
        return jnp.repeat(jnp.exp(steps), shape[dim] // shards_of).reshape((-1,) + (1,) * (len(shape) - dim - 1))

    level = one(*cuts[0])
    for cut in cuts[1:]:
        level = level * one(*cut)
    return level


def normal_values(key, dims, width, most, shards=(), kind=jnp.bfloat16):
    result = width * jax.random.normal(key, dims, jnp.float32)
    if shards:
        result = result * block_levels(key, dims, shards, -0.22, 0.18)
    return jnp.clip(result, -most, most).astype(kind)


def setup_inputs(seed: int = 0) -> dict:
    arg_keys = jax.random.split(jax.random.key(seed), 8)
    return {
        "resid": draw_resid(jax.random.fold_in(arg_keys[7], 71), 0),
        "norm_gain": jnp.clip(1.0 + 0.18 * jax.random.normal(arg_keys[1], (D,), jnp.float32), 0.1, 1.9),
        "w_gate": normal_values(arg_keys[2], (D, FF_WIN), D ** -0.5, 0.09375, ((1, 4),)),
        "w_up": normal_values(arg_keys[3], (D, FF_WIN), D ** -0.5, 0.09375, ((1, 4),)),
        "hit_neuron": draw_hit_neuron(jax.random.fold_in(arg_keys[7], 71), 0),
        "hit_start": draw_hit_start(jax.random.fold_in(arg_keys[7], 71), 0),
        "hit_mask": draw_hit_mask(jax.random.fold_in(arg_keys[7], 71), 0),
    }


EPS = 1e-05

def activations(rows, norm_gain, w_gate, w_up):
    values = rows.astype(jnp.float32)
    power = lax.optimization_barrier(jnp.mean(values * values, axis=-1, keepdims=True))
    normed = (values * lax.rsqrt(power + EPS) * norm_gain).astype(jnp.bfloat16)
    gate = jnp.dot(normed, w_gate, preferred_element_type=jnp.float32)
    upward = jnp.dot(normed, w_up, preferred_element_type=jnp.float32)
    return jax.nn.silu(gate) * upward

def reference(resid, norm_gain, w_gate, w_up, hit_neuron, hit_start, hit_mask):
    local_width = FF_WIN // N_NEUR

    def take_window(begin):
        return lax.dynamic_slice_in_dim(resid, begin, WIN, 0)

    def one_group(inputs):
        index, starts, masks, neurons = inputs
        block = (index % N_NEUR).astype(jnp.int32)
        first = (block * local_width).astype(jnp.int32)
        gate_cols = lax.dynamic_slice_in_dim(w_gate, first, local_width, 1)
        up_cols = lax.dynamic_slice_in_dim(w_up, first, local_width, 1)
        windows = jax.vmap(take_window)(starts)
        acts = activations(windows.reshape(HITS_DEV * WIN, D), norm_gain, gate_cols, up_cols).reshape(HITS_DEV, WIN, local_width)
        live = masks > 0
        coact = lax.optimization_barrier(jnp.max(jnp.where(live[:, :, None], acts, -jnp.inf), axis=1))
        local = (neurons - first).astype(jnp.int32)
        picked = jnp.take_along_axis(acts, local[:, None, None], axis=2)[:, :, 0]
        return (picked * masks.astype(jnp.float32), coact)
    groups = HITS // HITS_DEV
    profile, coact = lax.map(one_group, (jnp.arange(groups, dtype=jnp.int32), hit_start.reshape(groups, HITS_DEV), hit_mask.reshape(groups, HITS_DEV, WIN), hit_neuron.reshape(groups, HITS_DEV)))
    return (profile.reshape(HITS, WIN), coact.reshape(HITS, local_width))
```

```python
import functools

import jax
import jax.numpy as jnp
from jax import lax
from jax.experimental import pallas as pl
from jax.experimental.pallas import tpu as pltpu
from jax.sharding import PartitionSpec as P


EPS = 1e-05
GRAN = 8
LANES = 128
SENT = 4
FIELDS = 5
PIECES = (3, 4, 4, 3, 1, 1)
STRIP = 128
ROOM = 13 * 1024 * 1024
ROOM_STREAMED = 46 * 1024 * 1024


def norm_kernel(rows, gain, *outs, starts, counts):
    step = pl.program_id(0)
    strip = 16
    scale = gain[...].reshape(1, -1)

    for out, start, count in zip(outs, starts, counts):

        @pl.when((step >= start) & (step < start + count))
        def _():
            def one(i, carry):
                at = pl.multiple_of(i * strip, strip)
                values = rows[pl.ds(at, strip), :].astype(jnp.float32)
                power = jnp.mean(values * values, axis=-1, keepdims=True)
                scaled = values * lax.rsqrt(power + EPS) * scale
                out[pl.ds(at, strip), :] = scaled.astype(jnp.bfloat16)
                return carry

            lax.fori_loop(0, rows.shape[0] // strip, one, 0, unroll=2)


def norm_pieces(resid, gain, first_row, sizes, part):
    model_width = resid.shape[1]
    counts = [size // part for size in sizes]
    starts = [sum(counts[:i]) for i in range(len(sizes))]
    skip = first_row // part

    def piece_spec(start, count):
        return pl.BlockSpec((part, model_width), lambda j: (jnp.clip(j - start, 0, count - 1), 0))

    return pl.pallas_call(
        functools.partial(norm_kernel, starts=starts, counts=counts),
        grid=(sum(counts),),
        in_specs=[
            pl.BlockSpec((part, model_width), lambda j: (j + skip, 0)),
            pl.BlockSpec((model_width,), lambda j: (0,)),
        ],
        out_specs=[piece_spec(start, count) for start, count in zip(starts, counts)],
        out_shape=[jax.ShapeDtypeStruct((size, model_width), jnp.bfloat16) for size in sizes],
        compiler_params=pltpu.CompilerParams(
            dimension_semantics=("arbitrary",), vmem_limit_bytes=16 * 1024 * 1024
        ),
        name="norm_rows",
    )(resid, gain)


def block_kernel(table, order, bounds, *rest, spans, slots_rel, fresh, streamed):
    rows, rest = rest[:2 * len(spans)], rest[2 * len(spans):]
    w_gate, w_up, *rest = rest
    if fresh:
        before = None
        msg, acts, stack, sem = rest
    else:
        before, msg, acts, stack, sem = rest
    local_width = acts.shape[1]
    tile = w_gate.shape[1] if streamed else tile_of(local_width)
    slot_count = msg.shape[0]
    reach = acts.shape[0] - stack.shape[0]
    marks = bounds.shape[0] // 2
    listed = order.shape[0] // 2
    first_mark, last_mark = spans[0][0], spans[-1][0] + 1
    bases = [bounds[half * marks + first_mark] for half in range(2)]
    ends = [bounds[half * marks + last_mark] for half in range(2)]
    shifts = [0 - bases[0], ends[0] - bases[0] - bases[1]]
    total = ends[1] + shifts[1]

    def granule_copy(i, at, to):
        return pltpu.make_async_copy(
            rows[i].at[pl.ds(pl.multiple_of(at * GRAN, GRAN), GRAN), :],
            stack.at[pl.ds(pl.multiple_of(to * GRAN, GRAN), GRAN), :],
            sem,
        )

    def load_rows():
        for half in range(2):
            for i, (mark, first) in enumerate(spans):

                def one(rank, carry):
                    at = order[half * listed + rank] - first
                    granule_copy(half * len(spans) + i, at, rank + shifts[half]).start()
                    return carry

                lax.fori_loop(bounds[half * marks + mark], bounds[half * marks + mark + 1], one, 0)
        if fresh:
            msg[...] = jnp.full(msg.shape, -jnp.inf, jnp.float32)
        else:
            msg[...] = before[...]

        def settle(g, carry):
            granule_copy(0, 0, 0).wait()
            return carry

        lax.fori_loop(0, total, settle, 0)

    def one_tile(gate_tile, up_tile, at):
        columns = pl.ds(pl.multiple_of(at, tile), tile)

        def part(m, carry):
            span = pl.ds(pl.multiple_of(m * STRIP, STRIP), STRIP)
            gate = jnp.dot(stack[span, :], gate_tile(), preferred_element_type=jnp.float32)
            upward = jnp.dot(stack[span, :], up_tile(), preferred_element_type=jnp.float32)
            acts[span, columns] = gate / (1.0 + jnp.exp(-gate)) * upward
            return carry

        lax.fori_loop(0, (total * GRAN + STRIP - 1) // STRIP, part, 0)

    def read_hits():
        local = lax.broadcasted_iota(jnp.int32, (reach, 1), 0)
        lane = lax.broadcasted_iota(jnp.int32, (reach, LANES), 1)
        local_full = lax.broadcasted_iota(jnp.int32, (reach, LANES), 0)

        def one_slot(slot, carry):
            rank_low = table[slot * FIELDS]
            rank_high = table[slot * FIELDS + 1]
            second = (slot // slots_rel) % 2 == 1
            base = jnp.where(second, bases[1], bases[0])
            end = jnp.where(second, ends[1], ends[0])

            @pl.when((rank_high >= base) & (rank_low < end))
            def _():
                low = table[slot * FIELDS + 2]
                high = table[slot * FIELDS + 3]
                neuron = table[slot * FIELDS + 4]
                rank = jnp.maximum(rank_low, base)
                here = (jnp.minimum(rank_high + 1, end) - rank) * GRAN
                past = (rank - rank_low) * GRAN + low // GRAN * GRAN
                top = pl.multiple_of((rank + jnp.where(second, shifts[1], shifts[0])) * GRAN, GRAN)
                live = (local >= low - past) & (local <= high - past) & (local < here)
                best = jnp.max(jnp.where(live, acts[pl.ds(top, reach), :], -jnp.inf), axis=0, keepdims=True)
                column = pl.multiple_of(neuron // LANES * LANES, LANES)
                near = acts[pl.ds(top, reach), pl.ds(column, LANES)]
                picked = jnp.sum(jnp.where(lane == neuron % LANES, near, 0.0), axis=1, keepdims=True)
                mine = (lane == local_full + past) & (local_full < here)
                placed = jnp.max(jnp.where(mine, picked, -jnp.inf), axis=0, keepdims=True)
                found = jnp.concatenate([best, placed], axis=1)
                msg[pl.ds(slot, 1), :] = jnp.maximum(msg[pl.ds(slot, 1), :], found)

            return carry

        lax.fori_loop(0, slot_count, one_slot, 0)

    if streamed:
        step = pl.program_id(0)
        pl.when(step == 0)(load_rows)
        one_tile(lambda: w_gate[...], lambda: w_up[...], step * tile)
        pl.when(step == pl.num_programs(0) - 1)(read_hits)
    else:
        load_rows()

        def body(j, carry):
            columns = pl.ds(pl.multiple_of(j * tile, tile), tile)
            one_tile(lambda: w_gate[:, columns], lambda: w_up[:, columns], j * tile)
            return carry

        lax.fori_loop(0, local_width // tile, body, 0)
        read_hits()


def tile_of(local_width):
    return 256 if local_width % 256 == 0 else local_width


def run_block(plan, pieces, w_gate, w_up, before, width, slots_rel, streamed):
    table, order, bounds = plan
    model_width, local_width = w_gate.shape
    slot_count = table.shape[0] // FIELDS
    spans = [(mark, first // GRAN) for mark, first, _, _ in pieces]
    rows = [p[2] for p in pieces] + [p[3] for p in pieces]
    row_count = sum(r.shape[0] for r in rows)
    reach = (width + 2 * GRAN - 2) // GRAN * GRAN
    fresh = before is None
    msg_shape = (slot_count, local_width + LANES)
    if streamed:
        tile = tile_of(local_width)
        grid = (local_width // tile,)
        weight = pl.BlockSpec((model_width, tile), lambda j: (0, j))
        whole = pl.BlockSpec(msg_shape, lambda j: (0, 0))
    else:
        grid = ()
        weight = whole = pl.BlockSpec(memory_space=pltpu.VMEM)
    in_specs = [pl.BlockSpec(memory_space=pltpu.SMEM)] * 3
    in_specs += [pl.BlockSpec(memory_space=pltpu.HBM)] * len(rows)
    in_specs += [weight, weight]
    operands = [table, order, bounds, *rows, w_gate, w_up]
    aliases = {}
    if not fresh:
        in_specs.append(whole)
        operands.append(before)
        aliases = {len(operands) - 1: 0}
    return pl.pallas_call(
        functools.partial(
            block_kernel,
            spans=spans,
            slots_rel=slots_rel,
            fresh=fresh,
            streamed=streamed,
        ),
        grid=grid,
        in_specs=in_specs,
        out_specs=whole,
        out_shape=jax.ShapeDtypeStruct(msg_shape, jnp.float32),
        scratch_shapes=[
            pltpu.VMEM((row_count + reach, local_width), jnp.float32),
            pltpu.VMEM((row_count, model_width), jnp.bfloat16),
            pltpu.SemaphoreType.DMA,
        ],
        input_output_aliases=aliases,
        compiler_params=pltpu.CompilerParams(vmem_limit_bytes=ROOM_STREAMED if streamed else ROOM),
        cost_estimate=pl.CostEstimate(
            flops=2 * row_count * model_width * local_width,
            transcendentals=row_count * local_width,
            bytes_accessed=4 * model_width * local_width,
        ),
        name="block_acts",
    )(*operands)


def collect_kernel(where, shift, mask, *rest, phases, rows_each, local_width):
    parts = rest[:phases]
    profile, coact, whole = rest[phases:]
    for p in range(phases):
        whole[p * rows_each:(p + 1) * rows_each, :] = parts[p][...].astype(jnp.float32)
    width = profile.shape[1]

    def one(hit, carry):
        at = where[hit]
        row = whole[pl.ds(at, 1), :]
        coact[pl.ds(hit, 1), :] = row[:, :local_width]
        moved = pltpu.roll(jnp.broadcast_to(row[:, local_width:], (GRAN, LANES)), LANES - shift[hit], 1)
        profile[pl.ds(hit, 1), :] = jnp.where(mask[pl.ds(hit, 1), :] > 0, moved[:1, :width], 0.0)
        return carry

    lax.fori_loop(0, profile.shape[0], one, 0, unroll=8)


def collect(where, shift, mask, parts, local_width):
    own_hits, width = mask.shape
    rows_each = parts[0].shape[0]
    vmem = pl.BlockSpec(memory_space=pltpu.VMEM)
    smem = pl.BlockSpec(memory_space=pltpu.SMEM)
    return pl.pallas_call(
        functools.partial(collect_kernel, phases=len(parts), rows_each=rows_each, local_width=local_width),
        in_specs=[smem, smem, vmem] + [vmem] * len(parts),
        out_specs=(vmem, vmem),
        out_shape=(
            jax.ShapeDtypeStruct((own_hits, width), jnp.float32),
            jax.ShapeDtypeStruct((own_hits, local_width), jnp.float32),
        ),
        scratch_shapes=[pltpu.VMEM((len(parts) * rows_each, local_width + LANES), jnp.float32)],
        compiler_params=pltpu.CompilerParams(vmem_limit_bytes=16 * 1024 * 1024),
        name="collect_hits",
    )(where, shift, mask, *parts)


def in_hbm(x):
    return pltpu.with_memory_space_constraint(x, pltpu.HBM)


def per_device(resid, norm_gain, w_gate, w_up, hit_neuron, hit_start, hit_mask):
    resid = in_hbm(resid)
    width = hit_mask.shape[1]
    block_rows, _ = resid.shape
    groups = lax.axis_size("corpus")
    columns = lax.axis_size("neur")
    devices = groups * columns
    own_hits = hit_start.shape[0]
    local_width = w_gate.shape[1]
    slots = max(1, 2 * own_hits // devices)
    member = lax.axis_index("neur")
    chips = columns // 2
    gain = in_hbm(norm_gain)

    unit = block_rows // 16
    sizes = [unit * n for n in PIECES]
    firsts = [sum(sizes[:i]) for i in range(len(sizes))]
    own = norm_pieces(resid, gain, 0, sizes[:1], unit)
    own = own + norm_pieces(resid, gain, sizes[0], sizes[1:], unit)
    own = [in_hbm(piece) for piece in own]
    swap = [(i, i ^ 1) for i in range(columns)]
    far = []
    for s in range(1, chips):
        ring = [(i, (i + 2 * s) % columns) for i in range(columns)]
        pieces = []
        for piece in own:
            pieces.append(in_hbm(lax.ppermute(piece, "neur", ring)))
        far.append(pieces)
    sibling = [in_hbm(lax.ppermute(piece, "neur", swap)) for piece in own]

    owner = hit_start // block_rows
    owner_group = owner // columns
    owner_column = owner % columns
    phase = (member // 2 - owner_column // 2) % chips
    rel = (owner_column % 2) ^ (member % 2)
    position = jnp.arange(own_hits, dtype=jnp.int32)
    earlier = (owner[:, None] == owner[None, :]) & (position[None, :] < position[:, None])
    rank = jnp.sum(earlier.astype(jnp.int32), axis=1)
    target = ((owner_group * chips + phase) * 2 + rel) * slots + rank
    local_start = hit_start - owner * block_rows
    shift = local_start % GRAN
    live = hit_mask > 0
    steps = jnp.arange(width, dtype=jnp.int32)[None, :]
    low = jnp.min(jnp.where(live, steps, width), axis=1) + shift
    high = jnp.max(jnp.where(live, steps, -1), axis=1) + shift
    fields = jnp.stack([local_start + 1, low, high, hit_neuron - member * local_width], axis=1)
    placed = target[:, None] == jnp.arange(devices * slots, dtype=jnp.int32)[None, :]
    sheet = jnp.sum(jnp.where(placed[:, :, None], fields[:, None, :], 0), axis=0)
    sheet = lax.all_to_all(sheet.reshape(groups, -1), "corpus", split_axis=0, concat_axis=0, tiled=True)
    sheet = sheet.reshape(groups, chips * 2 * slots, SENT)
    sheet = sheet - jnp.array([1, 0, 0, 0], jnp.int32)

    def send_back(msg):
        msg = msg.astype(jnp.bfloat16).reshape(groups, 2 * slots, -1)
        msg = lax.all_to_all(msg, "corpus", split_axis=0, concat_axis=0, tiled=True)
        return msg.reshape(groups * 2 * slots, -1)

    block_granules = block_rows // GRAN
    sheet = jnp.swapaxes(sheet.reshape(groups, chips, 2, slots, SENT), 0, 1)
    valid = sheet[..., 0] >= 0
    lowest = sheet[..., 0] // GRAN + sheet[..., 1] // GRAN
    highest = sheet[..., 0] // GRAN + sheet[..., 2] // GRAN
    granules = jnp.arange(block_granules, dtype=jnp.int32)
    covers = valid[..., None] & (granules >= lowest[..., None]) & (granules <= highest[..., None])
    need = jnp.any(covers, axis=(1, 3))
    upto = jnp.sum((need[:, :, None, :] & (granules <= granules[:, None])).astype(jnp.int32), axis=-1)
    ranks = upto - need.astype(jnp.int32)
    hit = need[:, :, None, :] & (ranks[:, :, None, :] == granules[:, None])
    orders = jnp.sum(jnp.where(hit, granules, 0), axis=-1).reshape(chips, -1)
    marks = jnp.array([first // GRAN for first in firsts] + [block_granules], jnp.int32)
    bounds = jnp.sum((need[:, :, None, :] & (granules < marks[:, None])).astype(jnp.int32), axis=-1)
    bounds = bounds.reshape(chips, -1)
    before_low = need[:, None, :, None, :] & (granules < lowest[..., None])
    rank_low = jnp.sum(before_low.astype(jnp.int32), axis=-1)
    rank_high = rank_low + highest - lowest
    absent = 2 * block_granules
    tables = jnp.stack(
        [
            jnp.where(valid, rank_low, absent),
            jnp.where(valid, rank_high, -1),
            sheet[..., 1],
            sheet[..., 2],
            sheet[..., 3],
        ],
        axis=-1,
    ).reshape(chips, -1)
    plans = lax.optimization_barrier([(tables[s], orders[s], bounds[s]) for s in range(chips)])

    kept_gate = pltpu.with_memory_space_constraint(w_gate, pltpu.VMEM)
    kept_up = pltpu.with_memory_space_constraint(w_up, pltpu.VMEM)
    parts = []
    near_pieces = [(i, firsts[i], own[i], sibling[i]) for i in range(len(own))]
    near_msg = run_block(plans[0], near_pieces, in_hbm(w_gate), in_hbm(w_up), None, width, slots, True)
    done = [near_msg]
    for s in range(1, chips):
        msg = None
        for i, direct in enumerate(far[s - 1]):
            if s == 1 and i == len(own) // 2 - 1:
                near_msg, _ = lax.optimization_barrier((near_msg, done[-1]))
                parts.append(send_back(near_msg))
                direct, _ = lax.optimization_barrier((direct, parts[0]))
            direct, _ = lax.optimization_barrier((direct, done[-1]))
            relayed = lax.ppermute(direct, "neur", swap)
            relayed, _ = lax.optimization_barrier((in_hbm(relayed), done[-1]))
            piece = (i, firsts[i], direct, relayed)
            msg = run_block(plans[s], [piece], kept_gate, kept_up, msg, width, slots, False)
            done.append(msg)
        parts.append(send_back(msg))

    if chips == 1:
        parts.append(send_back(near_msg))
    where = (phase * groups + owner_group) * 2 * slots + rel * slots + rank
    return collect(where, shift, hit_mask, parts, local_width)


def solution(mesh):
    placed = (
        P(("corpus", "neur"), None),
        P(),
        P(None, "neur"),
        P(None, "neur"),
        P(("corpus", "neur")),
        P(("corpus", "neur")),
        P(("corpus", "neur"), None),
    )
    return jax.shard_map(
        per_device,
        mesh=mesh,
        in_specs=placed,
        out_specs=(P(("corpus", "neur"), None), P(("corpus", "neur"), None)),
        check_vma=False,
    )
```

```python
import functools

import jax
import jax.numpy as jnp
from jax import lax
from jax.experimental import pallas as pl
from jax.experimental.pallas import tpu as pltpu
from jax.sharding import PartitionSpec as P


EPS = 1e-05
GRAN = 8
LANES = 128
SENT = 4
FIELDS = 6
UNITS = 16
FLIP = 1 << 20
DENSE = 2
PACKED = (3, 3, 2, 1, 1)
STRIP = 128
ROOM = 13 * 1024 * 1024
ROOM_STREAMED = 46 * 1024 * 1024


def norm_kernel(rows, gain, *outs, starts, counts):
    step = pl.program_id(0)
    strip = 16
    scale = gain[...].reshape(1, -1)

    for out, start, count in zip(outs, starts, counts):

        @pl.when((step >= start) & (step < start + count))
        def _():
            def one(i, carry):
                at = pl.multiple_of(i * strip, strip)
                values = rows[pl.ds(at, strip), :].astype(jnp.float32)
                power = jnp.mean(values * values, axis=-1, keepdims=True)
                scaled = values * lax.rsqrt(power + EPS) * scale
                out[pl.ds(at, strip), :] = scaled.astype(jnp.bfloat16)
                return carry

            lax.fori_loop(0, rows.shape[0] // strip, one, 0, unroll=2)


def norm_pieces(resid, gain, first_row, sizes, part):
    model_width = resid.shape[1]
    counts = [size // part for size in sizes]
    starts = [sum(counts[:i]) for i in range(len(sizes))]
    skip = first_row // part

    def piece_spec(start, count):
        return pl.BlockSpec((part, model_width), lambda j: (jnp.clip(j - start, 0, count - 1), 0))

    return pl.pallas_call(
        functools.partial(norm_kernel, starts=starts, counts=counts),
        grid=(sum(counts),),
        in_specs=[
            pl.BlockSpec((part, model_width), lambda j: (j + skip, 0)),
            pl.BlockSpec((model_width,), lambda j: (0,)),
        ],
        out_specs=[piece_spec(start, count) for start, count in zip(starts, counts)],
        out_shape=[jax.ShapeDtypeStruct((size, model_width), jnp.bfloat16) for size in sizes],
        compiler_params=pltpu.CompilerParams(
            dimension_semantics=("arbitrary",), vmem_limit_bytes=16 * 1024 * 1024
        ),
        name="norm_rows",
    )(resid, gain)


def pack_kernel(listing, own, sibling, *rest, starts, block_granules):
    outs, sem = rest[:-1], rest[-1]

    def granule_copy(source, at, out, to):
        return pltpu.make_async_copy(
            source.at[pl.ds(pl.multiple_of(at * GRAN, GRAN), GRAN), :],
            out.at[pl.ds(pl.multiple_of(to * GRAN, GRAN), GRAN), :],
            sem,
        )

    for out, start in zip(outs, starts):

        def one(j, carry):
            at = listing[start + j]

            @pl.when(at < block_granules)
            def _():
                granule_copy(own, at, out, j).start()

            @pl.when(at >= block_granules)
            def _():
                granule_copy(sibling, at - block_granules, out, j).start()

            return carry

        lax.fori_loop(0, out.shape[0] // GRAN, one, 0)
    for out in outs:

        def settle(j, carry):
            granule_copy(own, 0, out, 0).wait()
            return carry

        lax.fori_loop(0, out.shape[0] // GRAN, settle, 0)


def pack_rows(listing, own, sibling, starts, sizes, block_granules):
    hbm = pl.BlockSpec(memory_space=pltpu.HBM)
    return pl.pallas_call(
        functools.partial(pack_kernel, starts=starts, block_granules=block_granules),
        in_specs=[pl.BlockSpec(memory_space=pltpu.SMEM), hbm, hbm],
        out_specs=[pl.BlockSpec(memory_space=pltpu.VMEM)] * len(sizes),
        out_shape=[jax.ShapeDtypeStruct((size * GRAN, own.shape[1]), own.dtype) for size in sizes],
        scratch_shapes=[pltpu.SemaphoreType.DMA],
        compiler_params=pltpu.CompilerParams(vmem_limit_bytes=20 * 1024 * 1024),
        name="pack_rows",
    )(listing, own, sibling)


def block_kernel(table, order, bounds, *rest, runs, fresh, streamed):
    row_refs = sum(len(run[2]) for run in runs)
    rows, rest = rest[:row_refs], rest[row_refs:]
    w_gate, w_up, *rest = rest
    if fresh:
        before = None
        msg, acts, stack, sem = rest
    else:
        before, msg, acts, stack, sem = rest
    local_width = acts.shape[1]
    tile = w_gate.shape[1] if streamed else tile_of(local_width)
    slot_count = msg.shape[0]
    reach = acts.shape[0] - stack.shape[0]
    base = bounds[runs[0][0]]
    end = bounds[runs[-1][0] + 1]
    total = end - base

    def granule_copy(i, at, to):
        return pltpu.make_async_copy(
            rows[i].at[pl.ds(pl.multiple_of(at * GRAN, GRAN), GRAN), :],
            stack.at[pl.ds(pl.multiple_of(to * GRAN, GRAN), GRAN), :],
            sem,
        )

    def load_rows():
        for mark, first, which in runs:

            def one(rank, carry):
                at = order[rank]
                if len(which) == 1:
                    granule_copy(which[0], at - first, rank - base).start()
                else:

                    @pl.when(at < FLIP)
                    def _():
                        granule_copy(which[0], at - first, rank - base).start()

                    @pl.when(at >= FLIP)
                    def _():
                        granule_copy(which[1], at - FLIP - first, rank - base).start()

                return carry

            lax.fori_loop(bounds[mark], bounds[mark + 1], one, 0)
        if fresh:
            msg[...] = jnp.full(msg.shape, -jnp.inf, jnp.float32)
        else:
            msg[...] = before[...]

        def settle(g, carry):
            granule_copy(0, 0, 0).wait()
            return carry

        lax.fori_loop(0, total, settle, 0)

    def one_tile(gate_tile, up_tile, at):
        columns = pl.ds(pl.multiple_of(at, tile), tile)

        def part(m, carry):
            span = pl.ds(pl.multiple_of(m * STRIP, STRIP), STRIP)
            gate = jnp.dot(stack[span, :], gate_tile(), preferred_element_type=jnp.float32)
            upward = jnp.dot(stack[span, :], up_tile(), preferred_element_type=jnp.float32)
            acts[span, columns] = gate / (1.0 + jnp.exp(-gate)) * upward
            return carry

        lax.fori_loop(0, (total * GRAN + STRIP - 1) // STRIP, part, 0)

    def read_hits():
        local = lax.broadcasted_iota(jnp.int32, (reach, 1), 0)
        lane = lax.broadcasted_iota(jnp.int32, (reach, LANES), 1)
        local_full = lax.broadcasted_iota(jnp.int32, (reach, LANES), 0)

        def one_slot(slot, carry):
            rank_low = table[slot * FIELDS]
            rank_high = table[slot * FIELDS + 1]

            @pl.when((rank_high >= base) & (rank_low < end))
            def _():
                low = table[slot * FIELDS + 3]
                high = table[slot * FIELDS + 4]
                neuron = table[slot * FIELDS + 5]
                rank = jnp.maximum(rank_low, base)
                here = (jnp.minimum(rank_high + 1, end) - rank) * GRAN
                past = (rank - rank_low) * GRAN + table[slot * FIELDS + 2]
                top = pl.multiple_of((rank - base) * GRAN, GRAN)
                live = (local >= low - past) & (local <= high - past) & (local < here)
                best = jnp.max(jnp.where(live, acts[pl.ds(top, reach), :], -jnp.inf), axis=0, keepdims=True)
                column = pl.multiple_of(neuron // LANES * LANES, LANES)
                near = acts[pl.ds(top, reach), pl.ds(column, LANES)]
                picked = jnp.sum(jnp.where(lane == neuron % LANES, near, 0.0), axis=1, keepdims=True)
                mine = (lane == local_full + past) & (local_full < here)
                placed = jnp.max(jnp.where(mine, picked, -jnp.inf), axis=0, keepdims=True)
                found = jnp.concatenate([best, placed], axis=1)
                msg[pl.ds(slot, 1), :] = jnp.maximum(msg[pl.ds(slot, 1), :], found)

            return carry

        lax.fori_loop(0, slot_count, one_slot, 0)

    if streamed:
        step = pl.program_id(0)
        pl.when(step == 0)(load_rows)
        one_tile(lambda: w_gate[...], lambda: w_up[...], step * tile)
        pl.when(step == pl.num_programs(0) - 1)(read_hits)
    else:
        load_rows()

        def body(j, carry):
            columns = pl.ds(pl.multiple_of(j * tile, tile), tile)
            one_tile(lambda: w_gate[:, columns], lambda: w_up[:, columns], j * tile)
            return carry

        lax.fori_loop(0, local_width // tile, body, 0)
        read_hits()


def tile_of(local_width):
    return 256 if local_width % 256 == 0 else local_width


def run_block(plan, pieces, w_gate, w_up, before, width, streamed):
    table, order, bounds = plan
    model_width, local_width = w_gate.shape
    slot_count = table.shape[0] // FIELDS
    rows = []
    runs = []
    for mark, first, sources in pieces:
        runs.append((mark, first, [len(rows) + i for i in range(len(sources))]))
        rows.extend(sources)
    row_count = sum(r.shape[0] for r in rows)
    reach = (width + 2 * GRAN - 2) // GRAN * GRAN
    fresh = before is None
    msg_shape = (slot_count, local_width + LANES)
    if streamed:
        tile = tile_of(local_width)
        grid = (local_width // tile,)
        weight = pl.BlockSpec((model_width, tile), lambda j: (0, j))
        whole = pl.BlockSpec(msg_shape, lambda j: (0, 0))
    else:
        grid = ()
        weight = whole = pl.BlockSpec(memory_space=pltpu.VMEM)
    in_specs = [pl.BlockSpec(memory_space=pltpu.SMEM)] * 3
    in_specs += [pl.BlockSpec(memory_space=pltpu.HBM)] * len(rows)
    in_specs += [weight, weight]
    operands = [table, order, bounds, *rows, w_gate, w_up]
    aliases = {}
    if not fresh:
        in_specs.append(whole)
        operands.append(before)
        aliases = {len(operands) - 1: 0}
    return pl.pallas_call(
        functools.partial(
            block_kernel,
            runs=runs,
            fresh=fresh,
            streamed=streamed,
        ),
        grid=grid,
        in_specs=in_specs,
        out_specs=whole,
        out_shape=jax.ShapeDtypeStruct(msg_shape, jnp.float32),
        scratch_shapes=[
            pltpu.VMEM((row_count + reach, local_width), jnp.float32),
            pltpu.VMEM((row_count, model_width), jnp.bfloat16),
            pltpu.SemaphoreType.DMA,
        ],
        input_output_aliases=aliases,
        compiler_params=pltpu.CompilerParams(vmem_limit_bytes=ROOM_STREAMED if streamed else ROOM),
        cost_estimate=pl.CostEstimate(
            flops=2 * row_count * model_width * local_width,
            transcendentals=row_count * local_width,
            bytes_accessed=4 * model_width * local_width,
        ),
        name="block_acts",
    )(*operands)


def collect_kernel(where, shift, mask, *rest, phases, rows_each, local_width):
    parts = rest[:phases]
    profile, coact, whole = rest[phases:]
    for p in range(phases):
        whole[p * rows_each:(p + 1) * rows_each, :] = parts[p][...].astype(jnp.float32)
    width = profile.shape[1]

    def one(hit, carry):
        at = where[hit]
        row = whole[pl.ds(at, 1), :]
        coact[pl.ds(hit, 1), :] = row[:, :local_width]
        moved = pltpu.roll(jnp.broadcast_to(row[:, local_width:], (GRAN, LANES)), LANES - shift[hit], 1)
        profile[pl.ds(hit, 1), :] = jnp.where(mask[pl.ds(hit, 1), :] > 0, moved[:1, :width], 0.0)
        return carry

    lax.fori_loop(0, profile.shape[0], one, 0, unroll=8)


def collect(where, shift, mask, parts, local_width):
    own_hits, width = mask.shape
    rows_each = parts[0].shape[0]
    vmem = pl.BlockSpec(memory_space=pltpu.VMEM)
    smem = pl.BlockSpec(memory_space=pltpu.SMEM)
    return pl.pallas_call(
        functools.partial(collect_kernel, phases=len(parts), rows_each=rows_each, local_width=local_width),
        in_specs=[smem, smem, vmem] + [vmem] * len(parts),
        out_specs=(vmem, vmem),
        out_shape=(
            jax.ShapeDtypeStruct((own_hits, width), jnp.float32),
            jax.ShapeDtypeStruct((own_hits, local_width), jnp.float32),
        ),
        scratch_shapes=[pltpu.VMEM((len(parts) * rows_each, local_width + LANES), jnp.float32)],
        compiler_params=pltpu.CompilerParams(vmem_limit_bytes=16 * 1024 * 1024),
        name="collect_hits",
    )(where, shift, mask, *parts)


def make_plan(flags, codes, cuts, starts, lengths, pasts, extra):
    places = jnp.arange(flags.shape[0], dtype=jnp.int32)
    ranks = jnp.sum((flags & (places < places[:, None])).astype(jnp.int32), axis=1)
    order = jnp.sum(jnp.where(flags & (ranks == places[:, None]), codes, 0), axis=1)
    bounds = jnp.sum((flags & cuts).astype(jnp.int32), axis=1)
    first = jnp.sum((flags & (places < starts[:, None])).astype(jnp.int32), axis=1)
    some = lengths > 0
    table = jnp.stack(
        [jnp.where(some, first, 2 * FLIP), jnp.where(some, first + lengths - 1, -1), pasts, *extra], axis=1
    )
    return table.reshape(-1), order, bounds


def in_hbm(x):
    return pltpu.with_memory_space_constraint(x, pltpu.HBM)


def per_device(resid, norm_gain, w_gate, w_up, hit_neuron, hit_start, hit_mask):
    resid = in_hbm(resid)
    width = hit_mask.shape[1]
    block_rows, _ = resid.shape
    groups = lax.axis_size("corpus")
    columns = lax.axis_size("neur")
    devices = groups * columns
    own_hits = hit_start.shape[0]
    local_width = w_gate.shape[1]
    slots = max(1, 2 * own_hits // devices)
    member = lax.axis_index("neur")
    chips = columns // 2
    gain = in_hbm(norm_gain)

    unit = block_rows // UNITS
    dense_rows = DENSE * unit
    own_first = norm_pieces(resid, gain, 0, [dense_rows], unit)[0]
    own_rest = norm_pieces(resid, gain, dense_rows, [block_rows - dense_rows], dense_rows)[0]
    own_first, own_rest = in_hbm(own_first), in_hbm(own_rest)
    swap = [(i, i ^ 1) for i in range(columns)]

    def forward(s):
        return [(i, (i + 2 * s) % columns) for i in range(columns)]

    far_first = []
    for s in range(1, chips):
        far_first.append(in_hbm(lax.ppermute(own_first, "neur", forward(s))))
    sibling_first = in_hbm(lax.ppermute(own_first, "neur", swap))
    sibling_rest = in_hbm(lax.ppermute(own_rest, "neur", swap))

    owner = hit_start // block_rows
    owner_group = owner // columns
    owner_column = owner % columns
    phase = (member // 2 - owner_column // 2) % chips
    rel = (owner_column % 2) ^ (member % 2)
    position = jnp.arange(own_hits, dtype=jnp.int32)
    earlier = (owner[:, None] == owner[None, :]) & (position[None, :] < position[:, None])
    rank = jnp.sum(earlier.astype(jnp.int32), axis=1)
    target = ((owner_group * chips + phase) * 2 + rel) * slots + rank
    local_start = hit_start - owner * block_rows
    shift = local_start % GRAN
    live = hit_mask > 0
    steps = jnp.arange(width, dtype=jnp.int32)[None, :]
    low = jnp.min(jnp.where(live, steps, width), axis=1) + shift
    high = jnp.max(jnp.where(live, steps, -1), axis=1) + shift
    fields = jnp.stack([local_start + 1, low, high, hit_neuron - member * local_width], axis=1)
    placed = target[:, None] == jnp.arange(devices * slots, dtype=jnp.int32)[None, :]
    sheet = jnp.sum(jnp.where(placed[:, :, None], fields[:, None, :], 0), axis=0)
    sheet = lax.all_to_all(sheet.reshape(groups, -1), "corpus", split_axis=0, concat_axis=0, tiled=True)
    sheet = sheet.reshape(groups, chips * 2 * slots, SENT)
    sheet = sheet - jnp.array([1, 0, 0, 0], jnp.int32)

    def send_back(msg):
        msg = msg.astype(jnp.bfloat16).reshape(groups, 2 * slots, -1)
        msg = lax.all_to_all(msg, "corpus", split_axis=0, concat_axis=0, tiled=True)
        return msg.reshape(groups * 2 * slots, -1)

    block_granules = block_rows // GRAN
    both = 2 * block_granules
    dense = dense_rows // GRAN
    core = member % 2
    sheet = jnp.swapaxes(sheet.reshape(groups, chips, 2, slots, SENT), 0, 1)
    valid = sheet[..., 0] >= 0
    lowest = sheet[..., 0] // GRAN + sheet[..., 1] // GRAN
    highest = sheet[..., 0] // GRAN + sheet[..., 2] // GRAN
    granules = jnp.arange(block_granules, dtype=jnp.int32)
    covers = valid[..., None] & (granules >= lowest[..., None]) & (granules <= highest[..., None])
    need = jnp.any(covers, axis=(1, 3))
    sides = jnp.broadcast_to(jnp.arange(2, dtype=jnp.int32)[:, None], (2, slots))
    sides = jnp.broadcast_to(sides, (groups, 2, slots)).reshape(-1)
    flat_valid = valid.reshape(chips, -1)
    flat_low = lowest.reshape(chips, -1)
    flat_high = highest.reshape(chips, -1)
    fields = sheet.reshape(chips, -1, SENT)
    extras = [[fields[s, :, 1], fields[s, :, 2], fields[s, :, 3]] for s in range(chips)]
    places = jnp.arange(both, dtype=jnp.int32)
    inside = places % block_granules

    by_core = jnp.where(core == 0, need, need[:, ::-1]).astype(jnp.int32)
    asked = by_core | lax.ppermute(by_core, "neur", swap)
    received = [
        lax.ppermute(asked[s], "neur", [(i, (i - 2 * s) % columns) for i in range(columns)]) for s in range(1, chips)
    ]
    sizes = [n * unit // GRAN for n in PACKED]
    starts = [sum(sizes[:i]) for i in range(len(sizes))]
    capacity = sum(sizes)
    spare = block_granules - dense - capacity
    listings = []
    most = jnp.int32(0)
    turn = jnp.arange(block_granules - dense, dtype=jnp.int32)
    for s in range(1, chips):
        flags = (received[s - 1].reshape(-1) > 0) & (inside >= dense)
        ranks = jnp.sum((flags & (places < places[:, None])).astype(jnp.int32), axis=1)
        most = jnp.maximum(most, jnp.sum(flags.astype(jnp.int32)))
        most = jnp.maximum(most, jnp.sum(((asked[s].reshape(-1) > 0) & (inside >= dense)).astype(jnp.int32)))
        source = inside - dense + jnp.where(places // block_granules == core, 0, block_granules)
        picks = flags & (ranks == (2 * turn + core)[:, None])
        listings.append(jnp.sum(jnp.where(picks, source, 0), axis=1))
    counts = jnp.broadcast_to(most, (groups, LANES))
    most = jnp.max(lax.all_to_all(counts, "corpus", split_axis=0, concat_axis=0, tiled=True))
    if chips > 2:
        most = lax.pmax(most, "neur")
    over = most > 2 * capacity

    cuts = jnp.stack([places < m for m in (0, dense, block_granules, block_granules + dense, both)])
    near_plan = make_plan(
        need[0].reshape(-1),
        inside,
        cuts,
        sides * block_granules + flat_low[0],
        jnp.where(flat_valid[0], flat_high[0] - flat_low[0] + 1, 0),
        fields[0, :, 1] // GRAN * GRAN,
        extras[0],
    )
    far_plans = []
    for s in range(1, chips):
        first_flags = need[s, :, :dense].reshape(-1)
        first_places = jnp.arange(2 * dense, dtype=jnp.int32)
        first_plan = make_plan(
            first_flags,
            first_places % dense,
            jnp.stack([first_places < m for m in (0, dense, 2 * dense)]),
            sides * dense + flat_low[s],
            jnp.where(flat_valid[s], jnp.minimum(flat_high[s], dense - 1) - flat_low[s] + 1, 0),
            fields[s, :, 1] // GRAN * GRAN,
            extras[s],
        )
        flags = (asked[s].reshape(-1) > 0) & (inside >= dense)
        ranks = jnp.sum((flags & (places < places[:, None])).astype(jnp.int32), axis=1)
        codes = ranks // 2 + jnp.where(ranks % 2 == core, 0, FLIP)
        begin = jnp.maximum(flat_low[s], dense)
        packed_plan = make_plan(
            (by_core[s].reshape(-1) > 0) & (inside >= dense),
            codes,
            jnp.stack([ranks // 2 < m for m in (*starts, capacity, both)]),
            (sides ^ core) * block_granules + begin,
            jnp.where(flat_valid[s], flat_high[s] - begin + 1, 0),
            (fields[s, :, 1] // GRAN + begin - flat_low[s]) * GRAN,
            extras[s],
        )
        far_plans.append((first_plan, packed_plan))
    near_plan, far_plans, listings = lax.optimization_barrier((near_plan, far_plans, listings))

    packed = []
    for s in range(1, chips):
        pieces = pack_rows(listings[s - 1], own_rest, sibling_rest, starts, sizes, block_granules)
        sent = []
        for piece in pieces:
            sent.append(in_hbm(lax.ppermute(in_hbm(piece), "neur", forward(s))))
        packed.append(sent)

    kept_gate = pltpu.with_memory_space_constraint(w_gate, pltpu.VMEM)
    kept_up = pltpu.with_memory_space_constraint(w_up, pltpu.VMEM)
    far_gate, far_up = in_hbm(w_gate), in_hbm(w_up)
    parts = []
    near_pieces = [
        (0, 0, [own_first]),
        (1, dense, [own_rest]),
        (2, 0, [sibling_first]),
        (3, dense, [sibling_rest]),
    ]
    near_msg = run_block(near_plan, near_pieces, far_gate, far_up, None, width, True)
    done = [near_msg]
    for s in range(1, chips):
        first_plan, packed_plan = far_plans[s - 1]
        direct, _ = lax.optimization_barrier((far_first[s - 1], done[-1]))
        relayed = lax.ppermute(direct, "neur", swap)
        if s == 1:
            parts.append(send_back(near_msg))
            relayed, _ = lax.optimization_barrier((relayed, parts[0]))
        pieces = [(0, 0, [direct]), (1, 0, [in_hbm(relayed)])]
        msg = run_block(first_plan, pieces, far_gate, far_up, None, width, True)

        def leftover(msg):
            piece = pack_rows(listings[s - 1], own_rest, sibling_rest, [capacity], [spare], block_granules)[0]
            direct = in_hbm(lax.ppermute(piece, "neur", forward(s)))
            relayed = in_hbm(lax.ppermute(direct, "neur", swap))
            pieces = [(len(sizes), capacity, [direct, relayed])]
            return run_block(packed_plan, pieces, far_gate, far_up, msg, width, True)

        msg = lax.cond(over, leftover, lambda m: m, msg)
        done.append(msg)
        for i, direct in enumerate(packed[s - 1]):
            direct, _ = lax.optimization_barrier((direct, done[-2]))
            relayed = lax.ppermute(direct, "neur", swap)
            relayed, _ = lax.optimization_barrier((in_hbm(relayed), done[-1]))
            pieces = [(i, starts[i], [direct, relayed])]
            msg = run_block(packed_plan, pieces, kept_gate, kept_up, msg, width, False)
            done.append(msg)
        parts.append(send_back(msg))

    if chips == 1:
        parts.append(send_back(near_msg))
    where = (phase * groups + owner_group) * 2 * slots + rel * slots + rank
    return collect(where, shift, hit_mask, parts, local_width)


def solution(mesh):
    placed = (
        P(("corpus", "neur"), None),
        P(),
        P(None, "neur"),
        P(None, "neur"),
        P(("corpus", "neur")),
        P(("corpus", "neur")),
        P(("corpus", "neur"), None),
    )
    return jax.shard_map(
        per_device,
        mesh=mesh,
        in_specs=placed,
        out_specs=(P(("corpus", "neur"), None), P(("corpus", "neur"), None)),
        check_vma=False,
    )
```
